32 devices in a mesh: dp: 2 (over x), tp: 16 (over y, z, core).
Axes of the slice: x: 2, y: 2, z: 4, core: 2. Of those that a mesh axis runs over, the one named last changes fastest.
Arguments:
- x: bfloat16 [128, 4096], P('dp'), parts along dimension 0
- k_cache: bfloat16 [128, 2048, 64, 64], P('dp', None, 'tp'), parts along dimension 0
- v_cache: bfloat16 [128, 2048, 64, 64], P('dp', None, 'tp'), parts along dimension 0
- gain_a: bfloat16 [4096], replicated
- wq: bfloat16 [4096, 4096], P(None, 'tp')
- wo: bfloat16 [4096, 4096], P('tp')
- gain_m: bfloat16 [4096], replicated
- w_gate: bfloat16 [4096, 10240], P(None, 'tp')
- w_up: bfloat16 [4096, 10240], P(None, 'tp')
- w_down: bfloat16 [10240, 4096], P('tp')
Outputs:
- output: bfloat16 [128, 4096], P('dp'), parts along dimension 0
There are 2 independent parts. The reference program is written for one: setup_inputs(seed, part) draws one part's arguments, and reference() takes and returns one part's arrays. A program takes and returns all parts, laid end to end along the dimension named above; an argument that names none is the same for every part.
All inputs are finite; a program needn't handle non-finite values.
Results may differ from the reference program's by a relative error of at most 0.017.
Values are sent between devices in bfloat16 or wider.
A program may use at most 2 GiB of HBM per device.

```python
import jax
import jax.numpy as jnp
from jax import lax

BATCH = 64
CACHE = 2048
D = 4096
HEADS = 64
KV_HEADS = 64
HEAD = 64
FF = 10240
THETA = 10000


def setup_inputs(seed: int = 0, part: int = 0) -> dict:
    kx, kc, kw, kn, kq, ko, km, kg, ku, kd = jax.random.split(jax.random.key(seed), 10)
    kx, kc, kw = (jax.random.fold_in(k, part) for k in (kx, kc, kw))

    def weights(key, rows, columns):
        return jax.random.normal(key, (rows, columns), jnp.float32) * rows**-0.5

    drawn = {
        "x": jax.random.normal(kx, (BATCH, D), jnp.float32),
        "k_cache": 2 * jax.random.normal(kc, (BATCH, CACHE, KV_HEADS, HEAD), jnp.float32),
        "v_cache": 4 * jax.random.normal(kw, (BATCH, CACHE, KV_HEADS, HEAD), jnp.float32),
        "gain_a": 1 + 0.1 * jax.random.normal(kn, (D,), jnp.float32),
        "wq": 2 * weights(kq, D, HEADS * HEAD),
        "wo": weights(ko, HEADS * HEAD, D),
        "gain_m": 1 + 0.1 * jax.random.normal(km, (D,), jnp.float32),
        "w_gate": weights(kg, D, FF),
        "w_up": weights(ku, D, FF),
        "w_down": 2 * weights(kd, FF, D),
    }
    return {k: v.astype(jnp.bfloat16) for k, v in drawn.items()}


def normed(x, gain):
    wide = x.astype(jnp.float32)
    scale = lax.rsqrt(jnp.mean(wide * wide, -1, keepdims=True) + 1e-6)
    return (wide * scale * gain.astype(jnp.float32)).astype(jnp.bfloat16)


def turned(t, place, theta):
    half = t.shape[-1] // 2
    angle = place.astype(jnp.float32)[:, None] * theta ** (-jnp.arange(half, dtype=jnp.float32) / half)
    cos, sin = jnp.cos(angle)[:, None], jnp.sin(angle)[:, None]
    a, b = t[..., :half].astype(jnp.float32), t[..., half:].astype(jnp.float32)
    return jnp.concatenate([a * cos - b * sin, b * cos + a * sin], -1).astype(jnp.bfloat16)


def matmul(a, w):
    return jnp.dot(a, w, preferred_element_type=jnp.float32).astype(jnp.bfloat16)


def einsum(form, a, b):
    return jnp.einsum(form, a.astype(jnp.float32), b.astype(jnp.float32))


def seen_by(a, wq, k_cache, v_cache, head, theta):
    batch, cache, kv_heads = k_cache.shape[:3]
    place = jnp.full((batch,), cache - 1)
    q = turned(matmul(a, wq).reshape(batch, -1, head), place, theta).reshape(batch, kv_heads, -1, head)
    scores = einsum("bgsd,bugd->bgsu", q, k_cache) * head**-0.5
    weights = jax.nn.softmax(scores, -1).astype(jnp.bfloat16)
    return einsum("bgsu,bugd->bgsd", weights, v_cache).astype(jnp.bfloat16).reshape(batch, -1)


def hidden_of(b, w_gate, w_up):
    gate = jnp.dot(b, w_gate, preferred_element_type=jnp.float32)
    up = jnp.dot(b, w_up, preferred_element_type=jnp.float32)
    return (jax.nn.silu(gate) * up).astype(jnp.bfloat16)


def reference(x, k_cache, v_cache, gain_a, wq, wo, gain_m, w_gate, w_up, w_down):
    seen = seen_by(normed(x, gain_a), wq, k_cache, v_cache, HEAD, THETA)
    h = (x.astype(jnp.float32) + jnp.dot(seen, wo, preferred_element_type=jnp.float32)).astype(jnp.bfloat16)
    hidden = hidden_of(normed(h, gain_m), w_gate, w_up)
    return (h.astype(jnp.float32) + jnp.dot(hidden, w_down, preferred_element_type=jnp.float32)).astype(jnp.bfloat16)
```

```python
import functools

import jax
import jax.numpy as jnp
import numpy as np
from jax import lax
from jax.experimental import pallas as pl
from jax.experimental.pallas import tpu as pltpu
from jax.sharding import PartitionSpec as P

HEAD = 64
THETA = 10000
BF16, F32 = jnp.bfloat16, jnp.float32

N = 16
D = 4096
W = D // N
HL = 4
QW = HL * HEAD
FL = 640
B = 64
U = 2048
G = 4
NC = B // G
NS = 4
R = 16
NG = B // R
CPG = R // G
LAG = 3
TICKS = NC + 4 * LAG


def tables():
    half = HEAD // 2
    angle = np.float32(U - 1) * np.float32(THETA) ** (-np.arange(half, dtype=np.float32) / np.float32(half))
    cos, sin = np.cos(angle.astype(np.float64)), np.sin(angle.astype(np.float64))
    cos = np.tile(np.concatenate([cos, cos]), HL)
    sin = np.tile(np.concatenate([-sin, sin]), HL)
    return np.stack([np.broadcast_to(cos, (8, QW)), np.broadcast_to(sin, (8, QW))]).astype(np.float32)


def kernel(
    x_hbm, k_hbm, v_hbm, ga_hbm, wq_hbm, wo_hbm, gm_hbm, wg_hbm, wu_hbm, wd_hbm, cs_hbm, out_hbm,
    xs, ab, qbd, wq, wo, wgu, wd, ga, gm, cs, kbuf, vbuf, wts, seen, bs,
    send1, recv1, hs, send2, recv2, ys,
    misc_sem, ksem, vsem, wsem, osem, s1, r1, s2, r2, s3, r3, s4, r4,
):
    me = lax.axis_index("tp")
    barrier = pltpu.get_barrier_semaphore()
    for k in range(1, N):
        pl.semaphore_signal(barrier, inc=1, device_id={"tp": lax.rem(me + k, N)}, device_id_type=pl.DeviceIdType.MESH)

    def local(src, dst, sem):
        return pltpu.make_async_copy(src, dst, sem)

    def kcopy(c):
        rows = pl.ds(pl.multiple_of(c * (G * QW), G * QW), G * QW)
        return local(k_hbm.at[rows], kbuf.at[lax.rem(c, NS)], ksem.at[lax.rem(c, NS)])

    def vcopy(c):
        rows = pl.ds(pl.multiple_of(c * (G * QW), G * QW), G * QW)
        return local(v_hbm.at[rows], vbuf.at[lax.rem(c, NS)], vsem.at[lax.rem(c, NS)])

    first = [
        local(x_hbm, xs, misc_sem.at[0]),
        local(ga_hbm, ga, misc_sem.at[1]),
        local(wq_hbm, wq, misc_sem.at[2]),
        local(cs_hbm, cs, misc_sem.at[3]),
        local(gm_hbm, gm, misc_sem.at[4]),
    ]
    for c in first:
        c.start()
    for c in range(NS):
        kcopy(jnp.int32(c)).start()
        vcopy(jnp.int32(c)).start()
    wo_copy = local(wo_hbm, wo, wsem.at[0])
    wg_copy = local(wg_hbm, wgu.at[:, pl.ds(0, FL)], wsem.at[1])
    wu_copy = local(wu_hbm, wgu.at[:, pl.ds(FL, FL)], wsem.at[2])
    wd_copy = local(wd_hbm, wd, wsem.at[3])

    first[0].wait()
    first[1].wait()
    gain = ga[...].astype(F32)
    for r in range(0, B, R):
        wide = xs[r:r + R, :].astype(F32)
        scale = lax.rsqrt(jnp.mean(wide * wide, -1, keepdims=True) + 1e-6)
        for j in range(D // 128):
            cols = slice(128 * j, 128 * j + 128)
            ab[r:r + R, cols] = (wide[:, cols] * scale * gain[j:j + 1, :]).astype(BF16)
    first[2].wait()
    q = jnp.dot(ab[...], wq[...], preferred_element_type=F32).astype(BF16).astype(F32)
    first[3].wait()
    first[4].wait()
    lane = lax.broadcasted_iota(jnp.int32, (B, QW), 1)
    rot = jnp.where(lax.rem(lane, HEAD) < HEAD // 2, pltpu.roll(q, QW - HEAD // 2, 1), pltpu.roll(q, HEAD // 2, 1))
    cosines, sines = cs[0, 0:1, :], cs[1, 0:1, :]
    q = (q * cosines + rot * sines).astype(BF16).astype(F32)
    row = lax.broadcasted_iota(jnp.int32, (G * HL, QW), 0)
    col = lax.broadcasted_iota(jnp.int32, (G * HL, QW), 1)
    for c in range(NC):
        for i in range(G):
            line = jnp.broadcast_to(q[c * G + i:c * G + i + 1, :], (G * HL, QW))
            line = jnp.where(col // HEAD + HL * i == row, line, 0.0)
            qbd[c, :, QW * i:QW * (i + 1)] = line.astype(BF16)

    def scores(c):
        kcopy(c).wait()
        return jnp.dot(qbd[c], kbuf[lax.rem(c, NS)], preferred_element_type=F32)

    def softmax(s, c):
        top = jnp.max(s, -1, keepdims=True)
        p = jnp.exp((s - top) * HEAD**-0.5)
        wts[lax.rem(c, 2)] = (p / jnp.sum(p, -1, keepdims=True)).astype(BF16)

    def values(c):
        vcopy(c).wait()
        return lax.dot_general(wts[lax.rem(c, 2)], vbuf[lax.rem(c, NS)], (((1,), (1,)), ((), ())), preferred_element_type=F32)

    def keep(o, c):
        grp = c // CPG
        base = lax.rem(c, CPG) * G
        total = seen[grp]
        for i in range(G):
            part = o[:, QW * i:QW * (i + 1)]
            part = jnp.where(col // HEAD + HL * i == row, part, 0.0)
            line = jnp.broadcast_to(jnp.sum(part, 0, keepdims=True), (R, QW))
            total = jnp.where(row == base + i, line, total)
        seen[grp] = total

    def scatter(send, recv, ssem, rsem, g):
        for k in range(1, N):
            to = lax.rem(me + k, N)
            pltpu.make_async_remote_copy(
                src_ref=send.at[g, to], dst_ref=recv.at[g, k - 1], send_sem=ssem.at[g], recv_sem=rsem.at[g],
                device_id={"tp": to}, device_id_type=pl.DeviceIdType.MESH,
            ).start()

    def gather(buf, ssem, rsem, g):
        for k in range(1, N):
            to = lax.rem(me + k, N)
            pltpu.make_async_remote_copy(
                src_ref=buf.at[g, me], dst_ref=buf.at[g, me], send_sem=ssem.at[g], recv_sem=rsem.at[g],
                device_id={"tp": to}, device_id_type=pl.DeviceIdType.MESH,
            ).start()

    def arrived(buf, ssem, rsem, g):
        whole = buf.at[g, pl.ds(0, N - 1)]
        done = pltpu.make_async_remote_copy(
            src_ref=whole, dst_ref=whole, send_sem=ssem.at[g], recv_sem=rsem.at[g],
            device_id={"tp": lax.rem(me + 1, N)}, device_id_type=pl.DeviceIdType.MESH,
        )
        done.wait_send()
        done.wait_recv()

    def summed(send, recv, g):
        total = send[g, me].astype(F32)
        for k in range(N - 1):
            total = total + recv[g, k].astype(F32)
        return total

    def stage1(g):
        o = jnp.dot(seen[g].astype(BF16), wo[...], preferred_element_type=F32)
        for j in range(N):
            send1[g, j] = o[:, W * j:W * (j + 1)].astype(BF16)
        scatter(send1, recv1, s1, r1, g)

    def stage2(g):
        arrived(recv1, s1, r1, g)
        rows = pl.ds(pl.multiple_of(g * R, R), R)
        cols = pl.ds(pl.multiple_of(me * W, W), W)
        hs[g, me] = (xs[rows, cols].astype(F32) + summed(send1, recv1, g)).astype(BF16)
        gather(hs, s2, r2, g)

    def stage3(g):
        arrived(hs, s2, r2, g)
        square = jnp.zeros((R, W), F32)
        for j in range(N):
            wide = hs[g, j].astype(F32)
            square = square + wide * wide
        scale = lax.rsqrt(jnp.sum(square, -1, keepdims=True) * (1.0 / D) + 1e-6)
        gain = gm[...].astype(F32)
        for j in range(N):
            wide = hs[g, j].astype(F32) * scale
            for i in range(2):
                n = 2 * j + i
                bs[:, 128 * n:128 * n + 128] = (wide[:, 128 * i:128 * i + 128] * gain[n:n + 1, :]).astype(BF16)
        both = jnp.dot(bs[...], wgu[...], preferred_element_type=F32)
        gate, up = both[:, :FL], both[:, FL:]
        hidden = (gate * jax.nn.sigmoid(gate) * up).astype(BF16)
        o = jnp.dot(hidden, wd[...], preferred_element_type=F32)
        for j in range(N):
            send2[g, j] = o[:, W * j:W * (j + 1)].astype(BF16)
        scatter(send2, recv2, s3, r3, g)

    def stage4(g):
        arrived(recv2, s3, r3, g)
        ys[g, me] = (hs[g, me].astype(F32) + summed(send2, recv2, g)).astype(BF16)
        gather(ys, s4, r4, g)

    def stage5(g):
        arrived(ys, s4, r4, g)
        local(ys.at[g], out_hbm.at[g], osem.at[g]).start()

    softmax(scores(jnp.int32(0)), jnp.int32(0))
    kcopy(jnp.int32(NS)).start()

    def tick(t, carry):
        @pl.when(t < NC - 1)
        def _():
            s = scores(t + 1)
            o = values(t)
            softmax(s, t + 1)
            keep(o, t)

        @pl.when(t == NC - 1)
        def _():
            keep(values(t), t)

        @pl.when(t + 1 + NS < NC)
        def _():
            kcopy(t + 1 + NS).start()

        @pl.when(t + NS < NC)
        def _():
            vcopy(t + NS).start()

        for at, copy in ((0, wo_copy), (2, wg_copy), (4, wu_copy), (6, wd_copy)):
            pl.when(t == at)(copy.start)

        @pl.when(t == CPG - 1)
        def _():
            wo_copy.wait()
            pl.semaphore_wait(barrier, N - 1)

        @pl.when(t == CPG - 1 + 2 * LAG)
        def _():
            wg_copy.wait()
            wu_copy.wait()
            wd_copy.wait()

        for i, stage in enumerate((stage1, stage2, stage3, stage4, stage5)):
            since = t - (CPG - 1) - LAG * i
            due = (since >= 0) & (lax.rem(since, CPG) == 0) & (since < CPG * NG)
            pl.when(due)(functools.partial(stage, since // CPG))
        return carry

    lax.fori_loop(0, TICKS, tick, 0)
    for g in range(NG):
        local(ys.at[g], out_hbm.at[g], osem.at[g]).wait()


def layer(x, k_cache, v_cache, gain_a, wq, wo, gain_m, w_gate, w_up, w_down):
    k = jnp.transpose(k_cache, (0, 2, 3, 1)).reshape(B * QW, U)
    v = jnp.transpose(v_cache, (0, 2, 3, 1)).reshape(B * QW, U)
    dma, vmem = pltpu.SemaphoreType.DMA, pltpu.VMEM
    out = pl.pallas_call(
        kernel,
        out_shape=jax.ShapeDtypeStruct((NG, N, R, W), BF16),
        in_specs=[pl.BlockSpec(memory_space=pl.ANY)] * 11,
        out_specs=pl.BlockSpec(memory_space=pl.ANY),
        scratch_shapes=[
            vmem((B, D), BF16), vmem((B, D), BF16), vmem((NC, G * HL, G * QW), BF16),
            vmem((D, QW), BF16), vmem((QW, D), BF16), vmem((D, 2 * FL), BF16), vmem((FL, D), BF16),
            vmem((D // 128, 128), BF16), vmem((D // 128, 128), BF16), vmem((2, 8, QW), F32),
            vmem((NS, G * QW, U), BF16), vmem((NS, G * QW, U), BF16), vmem((2, G * HL, U), BF16),
            vmem((NG, R, QW), F32), vmem((R, D), BF16),
            vmem((NG, N, R, W), BF16), vmem((NG, N - 1, R, W), BF16), vmem((NG, N, R, W), BF16),
            vmem((NG, N, R, W), BF16), vmem((NG, N - 1, R, W), BF16), vmem((NG, N, R, W), BF16),
            dma((5,)), dma((NS,)), dma((NS,)), dma((4,)), dma((NG,)),
        ] + [dma((NG,))] * 8,
        compiler_params=pltpu.CompilerParams(collective_id=0, has_side_effects=True, vmem_limit_bytes=67043328),
        name="layer",
    )(x, k, v, gain_a.reshape(D // 128, 128), wq, wo, gain_m.reshape(D // 128, 128), w_gate, w_up, w_down, jnp.asarray(tables()))
    return out.transpose(0, 2, 1, 3).reshape(B, D)


def solution(mesh):
    states, cache, columns, rows_of = P("dp", None), P("dp", None, "tp", None), P(None, "tp"), P("tp", None)
    return jax.shard_map(
        layer,
        mesh=mesh,
        in_specs=(states, cache, cache, P(None), columns, rows_of, P(None), columns, columns, rows_of),
        out_specs=states,
        check_vma=False,
    )
```

```python
import functools

import jax
import jax.numpy as jnp
import numpy as np
from jax import lax
from jax.experimental import pallas as pl
from jax.experimental.pallas import tpu as pltpu
from jax.sharding import PartitionSpec as P

HEAD = 64
THETA = 10000
BF16, F32 = jnp.bfloat16, jnp.float32

N = 16
D = 4096
W = D // N
HL = 4
QW = HL * HEAD
FL = 640
B = 64
U = 2048
G = 4
NC = B // G
NS = 4
ROWS = (16, 16, 16, 8, 8)
NG = len(ROWS)
FIRST = tuple(sum(ROWS[:g]) for g in range(NG))
Q, Z = 4, 4
DURING = {
    3: ((1, 0),), 5: ((2, 0),), 7: ((1, 1), (3, 0)), 9: ((2, 1), (4, 0)), 11: ((1, 2), (3, 1), (5, 0)),
    13: ((1, 3), (2, 2)), 14: ((6, 0),), 15: ((1, 4), (3, 2), (2, 3)),
}
AFTER = (
    (4, 1), (2, 4), (7, 0), (3, 3), (4, 2), (5, 1), (3, 4), (4, 3), (5, 2), (4, 4), (6, 1), (5, 3), (6, 2), (5, 4),
    (7, 1), (6, 3), (7, 2), (6, 4), (7, 3), (7, 4),
)
LM = G * HL


def tables():
    half = HEAD // 2
    angle = np.float32(U - 1) * np.float32(THETA) ** (-np.arange(half, dtype=np.float32) / np.float32(half))
    cos, sin = np.cos(angle.astype(np.float64)), np.sin(angle.astype(np.float64))
    cos = np.tile(np.concatenate([cos, cos]), HL)
    sin = np.tile(np.concatenate([-sin, sin]), HL)
    return np.stack([np.broadcast_to(cos, (8, QW)), np.broadcast_to(sin, (8, QW))]).astype(np.float32)


def kernel(
    x_hbm, k_hbm, v_hbm, ga_hbm, wq_hbm, wo_hbm, gm_hbm, wg_hbm, wu_hbm, wd_hbm, cs_hbm, out,
    xs, ab, qbd, wq, wo, wgu, wd, ga, gm, cs, kbuf, vbuf, wts, seen, bs,
    misc_sem, ksem, vsem, wsem, ssem, rsem, *parts,
):
    terms1, near1, line1, hs, terms2, near2, line2, ys = (parts[NG * i:NG * (i + 1)] for i in range(8))
    me = lax.axis_index("tp")
    barrier = pltpu.get_barrier_semaphore()
    for k in range(1, N):
        pl.semaphore_signal(barrier, inc=1, device_id={"tp": lax.rem(me + k, N)}, device_id_type=pl.DeviceIdType.MESH)

    def local(src, dst, sem):
        return pltpu.make_async_copy(src, dst, sem)

    def kcopy(c):
        rows = pl.ds(pl.multiple_of(c * (G * QW), G * QW), G * QW)
        return local(k_hbm.at[rows], kbuf.at[lax.rem(c, NS)], ksem.at[lax.rem(c, NS)])

    def vcopy(c):
        rows = pl.ds(pl.multiple_of(c * (G * QW), G * QW), G * QW)
        return local(v_hbm.at[rows], vbuf.at[lax.rem(c, NS)], vsem.at[lax.rem(c, NS)])

    first = [
        local(x_hbm, xs, misc_sem.at[0]),
        local(ga_hbm, ga, misc_sem.at[1]),
        local(wq_hbm, wq, misc_sem.at[2]),
        local(cs_hbm, cs, misc_sem.at[3]),
        local(gm_hbm, gm, misc_sem.at[4]),
    ]
    for c in first:
        c.start()
    kcopy(jnp.int32(0)).start()
    wo_copy = local(wo_hbm, wo, wsem.at[0])
    wg_copy = local(wg_hbm, wgu.at[:, pl.ds(0, FL)], wsem.at[1])
    wu_copy = local(wu_hbm, wgu.at[:, pl.ds(FL, FL)], wsem.at[2])
    wd_copy = local(wd_hbm, wd, wsem.at[3])

    first[0].wait()
    first[1].wait()
    gain = ga[...].astype(F32)
    for r in range(0, B, 16):
        wide = xs[r:r + 16, :].astype(F32)
        scale = lax.rsqrt(jnp.mean(wide * wide, -1, keepdims=True) + 1e-6)
        for j in range(D // 128):
            cols = slice(128 * j, 128 * j + 128)
            ab[r:r + 16, cols] = (wide[:, cols] * scale * gain[j:j + 1, :]).astype(BF16)
    first[2].wait()
    vcopy(jnp.int32(0)).start()
    kcopy(jnp.int32(1)).start()
    vcopy(jnp.int32(1)).start()
    q = jnp.dot(ab[...], wq[...], preferred_element_type=F32).astype(BF16).astype(F32)
    first[3].wait()
    first[4].wait()
    lane = lax.broadcasted_iota(jnp.int32, (B, QW), 1)
    rot = jnp.where(lax.rem(lane, HEAD) < HEAD // 2, pltpu.roll(q, QW - HEAD // 2, 1), pltpu.roll(q, HEAD // 2, 1))
    cosines, sines = cs[0, 0:1, :], cs[1, 0:1, :]
    q = (q * cosines + rot * sines).astype(BF16).astype(F32)
    row = lax.broadcasted_iota(jnp.int32, (LM, QW), 0)
    col = lax.broadcasted_iota(jnp.int32, (LM, QW), 1)
    for c in range(NC):
        for i in range(G):
            line = jnp.broadcast_to(q[c * G + i:c * G + i + 1, :], (LM, QW))
            line = jnp.where(col // HEAD + HL * i == row, line, 0.0)
            qbd[c, :, QW * i:QW * (i + 1)] = line.astype(BF16)

    def scores(c):
        kcopy(c).wait()
        return jnp.dot(qbd[c], kbuf[lax.rem(c, NS)], preferred_element_type=F32)

    def softmax(s, c):
        top = jnp.max(s, -1, keepdims=True)
        p = jnp.exp((s - top) * HEAD**-0.5)
        wts[lax.rem(c, 2)] = (p / jnp.sum(p, -1, keepdims=True)).astype(BF16)

    def values(c):
        vcopy(c).wait()
        return lax.dot_general(wts[lax.rem(c, 2)], vbuf[lax.rem(c, NS)], (((1,), (1,)), ((), ())), preferred_element_type=F32)

    def keep(o, c):
        block = lax.div(c * G, 8)
        base = lax.rem(c * G, 8)
        total = seen[block]
        sub = lax.broadcasted_iota(jnp.int32, (8, QW), 0)
        for i in range(G):
            part = o[:, QW * i:QW * (i + 1)]
            part = jnp.where(col // HEAD + HL * i == row, part, 0.0)
            line = jnp.broadcast_to(jnp.sum(part, 0, keepdims=True), (8, QW))
            total = jnp.where(sub == base + i, line, total)
        seen[block] = total

    y, z, core = me // 8, lax.rem(me // 2, Z), lax.rem(me, 2)
    mine = y * 2 + core

    def send(src, dst, phase, g, to):
        pltpu.make_async_remote_copy(
            src_ref=src, dst_ref=dst, send_sem=ssem.at[phase, g], recv_sem=rsem.at[phase, g],
            device_id={"tp": to}, device_id_type=pl.DeviceIdType.MESH,
        ).start()

    def arrived(whole, phase, g):
        done = pltpu.make_async_remote_copy(
            src_ref=whole, dst_ref=whole, send_sem=ssem.at[phase, g], recv_sem=rsem.at[phase, g],
            device_id={"tp": lax.rem(me + 1, N)}, device_id_type=pl.DeviceIdType.MESH,
        )
        done.wait_send()
        done.wait_recv()

    def in_plane(k):
        other = lax.rem(mine + k, Q)
        return other, (other // 2) * 8 + z * 2 + lax.rem(other, 2)

    def scatter(terms, near, phase, g):
        for k in range(1, Q):
            other, to = in_plane(k)
            send(terms[g].at[pl.ds(other * Q, Q)], near[g].at[k - 1], phase, g, to)

    def along(terms, near, line, phase, g):
        arrived(near[g], phase, g)
        for j in range(Q):
            total = terms[g][mine * Q + j].astype(F32)
            for k in range(Q - 1):
                total = total + near[g][k, j].astype(F32)
            line[g][z, j] = total.astype(BF16)
        for k in range(1, Z):
            send(line[g].at[z], line[g].at[z], phase + 1, g, y * 8 + lax.rem(z + k, Z) * 2 + core)

    def gather(line, buf, residual, phase, g):
        arrived(line[g].at[pl.ds(0, Z - 1)], phase + 1, g)
        for j in range(Q):
            total = line[g][0, j].astype(F32)
            for k in range(1, Z):
                total = total + line[g][k, j].astype(F32)
            buf[g][mine * Q + j] = (residual(j) + total).astype(BF16)
        for k in range(1, Q):
            _, to = in_plane(k)
            own = buf[g].at[pl.ds(mine * Q, Q)]
            send(own, own, phase + 2, g, to)

    def gathered(buf, phase, g):
        arrived(buf[g].at[pl.ds(0, N - Q)], phase + 2, g)

    def stage1(g):
        rows = seen[FIRST[g] // 8:(FIRST[g] + ROWS[g]) // 8].reshape(ROWS[g], QW)
        o = jnp.dot(rows.astype(BF16), wo[...], preferred_element_type=F32)
        for j in range(N):
            terms1[g][j] = o[:, W * j:W * (j + 1)].astype(BF16)
        scatter(terms1, near1, 0, g)

    def stage2(g):
        along(terms1, near1, line1, 0, g)

    def stage3(g):
        def residual(j):
            cols = pl.ds(pl.multiple_of((mine * Q + j) * W, W), W)
            return xs[FIRST[g]:FIRST[g] + ROWS[g], cols].astype(F32)

        gather(line1, hs, residual, 0, g)

    def stage4(g):
        gathered(hs, 0, g)
        square = jnp.zeros((ROWS[g], W), F32)
        for j in range(N):
            wide = hs[g][j].astype(F32)
            square = square + wide * wide
        scale = lax.rsqrt(jnp.sum(square, -1, keepdims=True) * (1.0 / D) + 1e-6)
        gain = gm[...].astype(F32)
        for j in range(N):
            wide = hs[g][j].astype(F32) * scale
            for i in range(2):
                n = 2 * j + i
                bs[:ROWS[g], 128 * n:128 * n + 128] = (wide[:, 128 * i:128 * i + 128] * gain[n:n + 1, :]).astype(BF16)
        both = jnp.dot(bs[:ROWS[g], :], wgu[...], preferred_element_type=F32)
        gate, up = both[:, :FL], both[:, FL:]
        hidden = (gate * jax.nn.sigmoid(gate) * up).astype(BF16)
        o = jnp.dot(hidden, wd[...], preferred_element_type=F32)
        for j in range(N):
            terms2[g][j] = o[:, W * j:W * (j + 1)].astype(BF16)
        scatter(terms2, near2, 3, g)

    def stage5(g):
        along(terms2, near2, line2, 3, g)

    def stage6(g):
        gather(line2, ys, lambda j: hs[g][mine * Q + j].astype(F32), 3, g)

    def stage7(g):
        gathered(ys, 3, g)
        for j in range(N):
            out[FIRST[g]:FIRST[g] + ROWS[g], W * j:W * (j + 1)] = ys[g][j]

    kcopy(jnp.int32(2)).start()
    vcopy(jnp.int32(2)).start()
    softmax(scores(jnp.int32(0)), jnp.int32(0))
    kcopy(jnp.int32(3)).start()
    vcopy(jnp.int32(3)).start()
    kcopy(jnp.int32(NS)).start()

    def tick(t, carry):
        @pl.when(t < NC - 1)
        def _():
            s = scores(t + 1)
            o = values(t)
            softmax(s, t + 1)
            keep(o, t)

        @pl.when(t == NC - 1)
        def _():
            keep(values(t), t)

        @pl.when(t + 1 + NS < NC)
        def _():
            kcopy(t + 1 + NS).start()

        @pl.when(t + NS < NC)
        def _():
            vcopy(t + NS).start()

        for at, copy in ((0, wo_copy), (2, wg_copy), (4, wu_copy), (6, wd_copy)):
            pl.when(t == at)(copy.start)

        for at, due in DURING.items():
            @pl.when(t == at)
            def _(due=due):
                if (1, 0) in due:
                    wo_copy.wait()
                    pl.semaphore_wait(barrier, N - 1)
                if (4, 0) in due:
                    wg_copy.wait()
                    wu_copy.wait()
                    wd_copy.wait()
                for n, g in due:
                    stages[n - 1](g)
        return carry

    stages = (stage1, stage2, stage3, stage4, stage5, stage6, stage7)
    lax.fori_loop(0, NC, tick, 0)
    for n, g in AFTER:
        stages[n - 1](g)


def layer(x, k_cache, v_cache, gain_a, wq, wo, gain_m, w_gate, w_up, w_down):
    k = jnp.transpose(k_cache, (0, 2, 3, 1)).reshape(B * QW, U)
    v = jnp.transpose(v_cache, (0, 2, 3, 1)).reshape(B * QW, U)
    dma, vmem = pltpu.SemaphoreType.DMA, pltpu.VMEM
    return pl.pallas_call(
        kernel,
        out_shape=pltpu.VMEM((B, D), BF16),
        in_specs=[pl.BlockSpec(memory_space=pl.ANY)] * 11,
        out_specs=pl.BlockSpec(memory_space=pltpu.VMEM),
        scratch_shapes=[
            vmem((B, D), BF16), vmem((B, D), BF16), vmem((NC, LM, G * QW), BF16),
            vmem((D, QW), BF16), vmem((QW, D), BF16), vmem((D, 2 * FL), BF16), vmem((FL, D), BF16),
            vmem((D // 128, 128), BF16), vmem((D // 128, 128), BF16), vmem((2, 8, QW), F32),
            vmem((NS, G * QW, U), BF16), vmem((NS, G * QW, U), BF16), vmem((2, LM, U), BF16),
            vmem((B // 8, 8, QW), F32), vmem((max(ROWS), D), BF16),
            dma((5,)), dma((NS,)), dma((NS,)), dma((4,)),
            dma((6, NG)), dma((6, NG)),
        ] + [vmem((*n, r, W), BF16) for n in ((N,), (Q - 1, Q), (Z, Q), (N,)) * 2 for r in ROWS],
        compiler_params=pltpu.CompilerParams(collective_id=0, has_side_effects=True, vmem_limit_bytes=65994752),
        name="layer",
    )(x, k, v, gain_a.reshape(D // 128, 128), wq, wo, gain_m.reshape(D // 128, 128), w_gate, w_up, w_down, jnp.asarray(tables()))


def solution(mesh):
    states, cache, columns, rows_of = P("dp", None), P("dp", None, "tp", None), P(None, "tp"), P("tp", None)
    return jax.shard_map(
        layer,
        mesh=mesh,
        in_specs=(states, cache, cache, P(None), columns, rows_of, P(None), columns, columns, rows_of),
        out_specs=states,
        check_vma=False,
    )
```

```python
import functools

import jax
import jax.numpy as jnp
import numpy as np
from jax import lax
from jax.experimental import pallas as pl
from jax.experimental.pallas import tpu as pltpu
from jax.sharding import PartitionSpec as P

HEAD = 64
THETA = 10000
BF16, F32 = jnp.bfloat16, jnp.float32

N = 16
D = 4096
W = D // N
HL = 4
QW = HL * HEAD
FL = 640
B = 64
U = 2048
G = 4
NC = B // G
NS = 4
ROWS = (16, 16, 16, 8, 8)
NG = len(ROWS)
FIRST = tuple(sum(ROWS[:g]) for g in range(NG))
Q, Z = 4, 4
DURING = {
    3: ((1, 0),), 5: ((2, 0),), 7: ((1, 1), (3, 0)), 9: ((2, 1), (4, 0)), 11: ((1, 2), (3, 1), (5, 0)),
    13: ((1, 3), (2, 2)), 14: ((6, 0),), 15: ((1, 4), (3, 2), (2, 3)),
}
AFTER = (
    (4, 1), (2, 4), (7, 0), (3, 3), (4, 2), (5, 1), (3, 4), (4, 3), (5, 2), (4, 4), (6, 1), (5, 3), (6, 2), (5, 4),
    (7, 1), (6, 3), (7, 2), (6, 4), (7, 3), (7, 4),
)
LM = G * HL


def tables():
    half = HEAD // 2
    angle = np.float32(U - 1) * np.float32(THETA) ** (-np.arange(half, dtype=np.float32) / np.float32(half))
    cos, sin = np.cos(angle.astype(np.float64)), np.sin(angle.astype(np.float64))
    cos = np.tile(np.concatenate([cos, cos]), HL)
    sin = np.tile(np.concatenate([-sin, sin]), HL)
    return np.stack([np.broadcast_to(cos, (8, QW)), np.broadcast_to(sin, (8, QW))]).astype(np.float32)


def kernel(
    x_hbm, k_hbm, v_hbm, ga_hbm, wq_hbm, wo_hbm, gm_hbm, wg_hbm, wu_hbm, wd_hbm, cs_hbm, out,
    xs, ab, qbd, wq, wo, wgu, wd, ga, gm, cs, kbuf, vbuf, wts, seen, bs,
    misc_sem, ksem, vsem, wsem, ssem, rsem, *parts,
):
    terms1, near1, line1, hs, terms2, near2, line2, ys = (parts[NG * i:NG * (i + 1)] for i in range(8))
    far1, far2 = parts[8 * NG:]
    me = lax.axis_index("tp")
    barrier = pltpu.get_barrier_semaphore()
    for k in range(1, N):
        pl.semaphore_signal(barrier, inc=1, device_id={"tp": lax.rem(me + k, N)}, device_id_type=pl.DeviceIdType.MESH)

    def local(src, dst, sem):
        return pltpu.make_async_copy(src, dst, sem)

    def kcopy(c):
        rows = pl.ds(pl.multiple_of(c * (G * QW), G * QW), G * QW)
        return local(k_hbm.at[rows], kbuf.at[lax.rem(c, NS)], ksem.at[lax.rem(c, NS)])

    def vcopy(c):
        rows = pl.ds(pl.multiple_of(c * (G * QW), G * QW), G * QW)
        return local(v_hbm.at[rows], vbuf.at[lax.rem(c, NS)], vsem.at[lax.rem(c, NS)])

    first = [
        local(x_hbm, xs, misc_sem.at[0]),
        local(ga_hbm, ga, misc_sem.at[1]),
        local(wq_hbm, wq, misc_sem.at[2]),
        local(cs_hbm, cs, misc_sem.at[3]),
        local(gm_hbm, gm, misc_sem.at[4]),
    ]
    for c in first:
        c.start()
    kcopy(jnp.int32(0)).start()
    wo_copy = local(wo_hbm, wo, wsem.at[0])
    wg_copy = local(wg_hbm, wgu.at[:, pl.ds(0, FL)], wsem.at[1])
    wu_copy = local(wu_hbm, wgu.at[:, pl.ds(FL, FL)], wsem.at[2])
    wd_copy = local(wd_hbm, wd, wsem.at[3])

    first[0].wait()
    first[1].wait()
    gain = ga[...].astype(F32)
    for r in range(0, B, 16):
        wide = xs[r:r + 16, :].astype(F32)
        scale = lax.rsqrt(jnp.mean(wide * wide, -1, keepdims=True) + 1e-6)
        for j in range(D // 128):
            cols = slice(128 * j, 128 * j + 128)
            ab[r:r + 16, cols] = (wide[:, cols] * scale * gain[j:j + 1, :]).astype(BF16)
    first[2].wait()
    vcopy(jnp.int32(0)).start()
    kcopy(jnp.int32(1)).start()
    vcopy(jnp.int32(1)).start()
    q = jnp.dot(ab[...], wq[...], preferred_element_type=F32).astype(BF16).astype(F32)
    first[3].wait()
    first[4].wait()
    lane = lax.broadcasted_iota(jnp.int32, (B, QW), 1)
    rot = jnp.where(lax.rem(lane, HEAD) < HEAD // 2, pltpu.roll(q, QW - HEAD // 2, 1), pltpu.roll(q, HEAD // 2, 1))
    cosines, sines = cs[0, 0:1, :], cs[1, 0:1, :]
    q = (q * cosines + rot * sines).astype(BF16).astype(F32)
    row = lax.broadcasted_iota(jnp.int32, (LM, QW), 0)
    col = lax.broadcasted_iota(jnp.int32, (LM, QW), 1)
    for c in range(NC):
        for i in range(G):
            line = jnp.broadcast_to(q[c * G + i:c * G + i + 1, :], (LM, QW))
            line = jnp.where(col // HEAD + HL * i == row, line, 0.0)
            qbd[c, :, QW * i:QW * (i + 1)] = line.astype(BF16)

    def scores(c):
        kcopy(c).wait()
        return jnp.dot(qbd[c], kbuf[lax.rem(c, NS)], preferred_element_type=F32)

    def softmax(s, c):
        top = jnp.max(s, -1, keepdims=True)
        p = jnp.exp((s - top) * HEAD**-0.5)
        wts[lax.rem(c, 2)] = (p / jnp.sum(p, -1, keepdims=True)).astype(BF16)

    def values(c):
        vcopy(c).wait()
        return lax.dot_general(wts[lax.rem(c, 2)], vbuf[lax.rem(c, NS)], (((1,), (1,)), ((), ())), preferred_element_type=F32)

    def keep(o, c):
        block = lax.div(c * G, 8)
        base = lax.rem(c * G, 8)
        total = seen[block]
        sub = lax.broadcasted_iota(jnp.int32, (8, QW), 0)
        for i in range(G):
            part = o[:, QW * i:QW * (i + 1)]
            part = jnp.where(col // HEAD + HL * i == row, part, 0.0)
            line = jnp.broadcast_to(jnp.sum(part, 0, keepdims=True), (8, QW))
            total = jnp.where(sub == base + i, line, total)
        seen[block] = total

    y, z, core = me // 8, lax.rem(me // 2, Z), lax.rem(me, 2)
    mine = y * 2 + core

    def send(src, dst, phase, g, to):
        pltpu.make_async_remote_copy(
            src_ref=src, dst_ref=dst, send_sem=ssem.at[phase, g], recv_sem=rsem.at[phase, g],
            device_id={"tp": to}, device_id_type=pl.DeviceIdType.MESH,
        ).start()

    def arrived(whole, phase, g):
        done = pltpu.make_async_remote_copy(
            src_ref=whole, dst_ref=whole, send_sem=ssem.at[phase, g], recv_sem=rsem.at[phase, g],
            device_id={"tp": lax.rem(me + 1, N)}, device_id_type=pl.DeviceIdType.MESH,
        )
        done.wait_send()
        done.wait_recv()

    def in_plane(k):
        other = lax.rem(mine + k, Q)
        return other, (other // 2) * 8 + z * 2 + lax.rem(other, 2)

    def scatter(terms, near, phase, g):
        for k in range(1, Q):
            other, to = in_plane(k)
            send(terms[g].at[pl.ds(other * Q, Q)], near[g].at[k - 1], phase, g, to)

    def along(terms, near, line, phase, g):
        arrived(near[g], phase, g)
        for j in range(Q):
            total = terms[g][mine * Q + j].astype(F32)
            for k in range(Q - 1):
                total = total + near[g][k, j].astype(F32)
            line[g][z, j] = total.astype(BF16)
        for k in range(1, Z):
            send(line[g].at[z], line[g].at[z], phase + 1, g, y * 8 + lax.rem(z + k, Z) * 2 + core)

    def gather(line, buf, residual, phase, g):
        arrived(line[g].at[pl.ds(0, Z - 1)], phase + 1, g)
        for j in range(Q):
            total = line[g][0, j].astype(F32)
            for k in range(1, Z):
                total = total + line[g][k, j].astype(F32)
            buf[g][mine * Q + j] = (residual(j) + total).astype(BF16)
        for k in range(1, Q):
            _, to = in_plane(k)
            own = buf[g].at[pl.ds(mine * Q, Q)]
            send(own, own, phase + 2, g, to)

    def gathered(buf, phase, g):
        arrived(buf[g].at[pl.ds(0, N - Q)], phase + 2, g)

    def scatter_all(terms, far, phase, g):
        for k in range(1, N):
            to = lax.rem(me + k, N)
            send(terms[g].at[to], far.at[k - 1], phase, g, to)

    def gather_all(terms, far, buf, residual, phase, g):
        arrived(far, phase, g)
        total = terms[g][me].astype(F32)
        for k in range(N - 1):
            total = total + far[k].astype(F32)
        buf[g][me] = (residual + total).astype(BF16)
        for k in range(1, N):
            send(buf[g].at[me], buf[g].at[me], phase + 2, g, lax.rem(me + k, N))

    def stage1(g):
        rows = seen[FIRST[g] // 8:(FIRST[g] + ROWS[g]) // 8].reshape(ROWS[g], QW)
        o = jnp.dot(rows.astype(BF16), wo[...], preferred_element_type=F32)
        for j in range(N):
            terms1[g][j] = o[:, W * j:W * (j + 1)].astype(BF16)
        scatter(terms1, near1, 0, g)

    def stage2(g):
        along(terms1, near1, line1, 0, g)

    def stage3(g):
        def residual(j):
            cols = pl.ds(pl.multiple_of((mine * Q + j) * W, W), W)
            return xs[FIRST[g]:FIRST[g] + ROWS[g], cols].astype(F32)

        gather(line1, hs, residual, 0, g)

    def stage4(g):
        gathered(hs, 0, g)
        square = jnp.zeros((ROWS[g], W), F32)
        for j in range(N):
            wide = hs[g][j].astype(F32)
            square = square + wide * wide
        scale = lax.rsqrt(jnp.sum(square, -1, keepdims=True) * (1.0 / D) + 1e-6)
        gain = gm[...].astype(F32)
        for j in range(N):
            wide = hs[g][j].astype(F32) * scale
            for i in range(2):
                n = 2 * j + i
                bs[:ROWS[g], 128 * n:128 * n + 128] = (wide[:, 128 * i:128 * i + 128] * gain[n:n + 1, :]).astype(BF16)
        both = jnp.dot(bs[:ROWS[g], :], wgu[...], preferred_element_type=F32)
        gate, up = both[:, :FL], both[:, FL:]
        hidden = (gate * jax.nn.sigmoid(gate) * up).astype(BF16)
        o = jnp.dot(hidden, wd[...], preferred_element_type=F32)
        for j in range(N):
            terms2[g][j] = o[:, W * j:W * (j + 1)].astype(BF16)
        if g == NG - 1:
            scatter_all(terms2, far2, 3, g)
        else:
            scatter(terms2, near2, 3, g)

    def stage5(g):
        if g == NG - 1:
            return gather_all(terms2, far2, ys, hs[g][me].astype(F32), 3, g)
        along(terms2, near2, line2, 3, g)

    def stage6(g):
        if g == NG - 1:
            return
        gather(line2, ys, lambda j: hs[g][mine * Q + j].astype(F32), 3, g)

    def stage7(g):
        if g == NG - 1:
            arrived(ys[g].at[pl.ds(0, N - 1)], 5, g)
        else:
            gathered(ys, 3, g)
        for j in range(N):
            out[FIRST[g]:FIRST[g] + ROWS[g], W * j:W * (j + 1)] = ys[g][j]

    kcopy(jnp.int32(2)).start()
    vcopy(jnp.int32(2)).start()
    softmax(scores(jnp.int32(0)), jnp.int32(0))
    kcopy(jnp.int32(3)).start()
    vcopy(jnp.int32(3)).start()
    kcopy(jnp.int32(NS)).start()

    def tick(t, carry):
        @pl.when(t < NC - 1)
        def _():
            s = scores(t + 1)
            o = values(t)
            softmax(s, t + 1)
            keep(o, t)

        @pl.when(t == NC - 1)
        def _():
            keep(values(t), t)

        @pl.when(t + 1 + NS < NC)
        def _():
            kcopy(t + 1 + NS).start()

        @pl.when(t + NS < NC)
        def _():
            vcopy(t + NS).start()

        for at, copy in ((0, wo_copy), (2, wg_copy), (4, wu_copy), (6, wd_copy)):
            pl.when(t == at)(copy.start)

        for at, due in DURING.items():
            @pl.when(t == at)
            def _(due=due):
                if (1, 0) in due:
                    wo_copy.wait()
                    pl.semaphore_wait(barrier, N - 1)
                if (4, 0) in due:
                    wg_copy.wait()
                    wu_copy.wait()
                    wd_copy.wait()
                for n, g in due:
                    stages[n - 1](g)
        return carry

    stages = (stage1, stage2, stage3, stage4, stage5, stage6, stage7)
    lax.fori_loop(0, NC, tick, 0)
    for n, g in AFTER:
        stages[n - 1](g)


def layer(x, k_cache, v_cache, gain_a, wq, wo, gain_m, w_gate, w_up, w_down):
    k = jnp.transpose(k_cache, (0, 2, 3, 1)).reshape(B * QW, U)
    v = jnp.transpose(v_cache, (0, 2, 3, 1)).reshape(B * QW, U)
    dma, vmem = pltpu.SemaphoreType.DMA, pltpu.VMEM
    return pl.pallas_call(
        kernel,
        out_shape=pltpu.VMEM((B, D), BF16),
        in_specs=[pl.BlockSpec(memory_space=pl.ANY)] * 11,
        out_specs=pl.BlockSpec(memory_space=pltpu.VMEM),
        scratch_shapes=[
            vmem((B, D), BF16), vmem((B, D), BF16), vmem((NC, LM, G * QW), BF16),
            vmem((D, QW), BF16), vmem((QW, D), BF16), vmem((D, 2 * FL), BF16), vmem((FL, D), BF16),
            vmem((D // 128, 128), BF16), vmem((D // 128, 128), BF16), vmem((2, 8, QW), F32),
            vmem((NS, G * QW, U), BF16), vmem((NS, G * QW, U), BF16), vmem((2, LM, U), BF16),
            vmem((B // 8, 8, QW), F32), vmem((max(ROWS), D), BF16),
            dma((5,)), dma((NS,)), dma((NS,)), dma((4,)),
            dma((6, NG)), dma((6, NG)),
        ] + [vmem((*n, r, W), BF16) for n in ((N,), (Q - 1, Q), (Z, Q), (N,)) * 2 for r in ROWS] + [vmem((N - 1, ROWS[-1], W), BF16)] * 2,
        compiler_params=pltpu.CompilerParams(collective_id=0, has_side_effects=True, vmem_limit_bytes=65994752),
        name="layer",
    )(x, k, v, gain_a.reshape(D // 128, 128), wq, wo, gain_m.reshape(D // 128, 128), w_gate, w_up, w_down, jnp.asarray(tables()))


def solution(mesh):
    states, cache, columns, rows_of = P("dp", None), P("dp", None, "tp", None), P(None, "tp"), P("tp", None)
    return jax.shard_map(
        layer,
        mesh=mesh,
        in_specs=(states, cache, cache, P(None), columns, rows_of, P(None), columns, columns, rows_of),
        out_specs=states,
        check_vma=False,
    )
```
